128 devices in a mesh: tm: 16 (over z_lo, y, core), chan: 8 (over x, z_hi).
Axes of the slice: x: 4, y: 4, z: 4 (z_hi: 2, z_lo: 2; z = z_hi * 2 + z_lo), core: 2. Of those that a mesh axis runs over, the one named last changes fastest.
Arguments:
- auxiliary: float32 [512, 524288], P('chan', 'tm'), may hold values from -30 to 30
- proofs: float32 [64, 524288], P('chan', 'tm'), may hold values from -12 to 12
Outputs:
- coherence: float32 [512, 64, 4096], P('chan', None, 'tm')
The draws below stay inside these ranges and needn't reach their ends.
All inputs are finite; a program needn't handle non-finite values.
Results may differ from the reference program's by a relative error of at most 0.00076.
Values may be sent and summed in bfloat16 or wider, within the bound.
No kernel may reach another device: no remote copies, remote signals or barrier semaphores. Data moves between devices by JAX's collectives and lax.ppermute only.
A program may use at most 192 MiB of HBM per device.

```python
import math
import jax
import jax.numpy as jnp
from jax import lax

AUX_CH = 512
WIT_CH = 64
SEG_LEN = 8192
STRIDE = 4096
BINS = 4096
SEGMENTS = 127
SAMPLES = 524288


def coupled_series(key):
    subkeys = [jax.random.fold_in(key, 101 + number) for number in range(9)]
    moments = jnp.arange(SAMPLES, dtype=jnp.float32) / SAMPLES
    wit_noise = jax.random.truncated_normal(subkeys[0], -6.0, 6.0, (WIT_CH, SAMPLES), jnp.float32)
    aux_noise = jax.random.truncated_normal(subkeys[1], -6.0, 6.0, (AUX_CH, SAMPLES), jnp.float32)
    spread = 1.0
    wit_offset = jax.random.uniform(subkeys[2], (WIT_CH,), jnp.float32, -spread, spread)
    proof_out = wit_noise + wit_offset[:, None] * (0.5 + moments)[None, :]
    target = jax.random.randint(subkeys[3], (AUX_CH,), 0, WIT_CH)
    delays = jax.random.randint(subkeys[4], (AUX_CH,), 0, 4)
    gains_aux = jax.random.uniform(subkeys[5], (AUX_CH,), jnp.float32, 0.0, 2.0)
    source = wit_noise[target]
    shifted = jax.vmap(lambda series_row, amount: jnp.roll(series_row, amount))(source, delays)
    aux_offset = jax.random.uniform(subkeys[6], (AUX_CH,), jnp.float32, -spread, spread)
    aux_out = aux_noise + gains_aux[:, None] * shifted + aux_offset[:, None] * (1.0 + 2.0 * moments)[None, :]
    return (aux_out, proof_out)


def draw_auxiliary(key, part):
    return coupled_series(key)[0]


def draw_proofs(key, part):
    return coupled_series(key)[1]


def setup_inputs(seed: int = 0) -> dict:
    seeds = jax.random.split(jax.random.key(seed), 3)
    auxiliary = draw_auxiliary(jax.random.fold_in(seeds[2], 71), 0)
    proofs = draw_proofs(jax.random.fold_in(seeds[2], 71), 0)
    return dict(auxiliary=auxiliary, proofs=proofs)


def spectra_of(series, channel_means):
    row_count = series.shape[0]
    blocks = series.reshape(row_count, SEGMENTS + 1, STRIDE)
    segments = jnp.concatenate([blocks[:, :-1], blocks[:, 1:]], axis=2)
    position = jnp.arange(SEG_LEN, dtype=jnp.float32)
    window = 0.5 - 0.5 * jnp.cos(2.0 * math.pi * position / SEG_LEN)
    windowed = (segments - channel_means[:, None, None]) * window
    spectrum = jnp.fft.rfft(windowed, axis=-1)[..., :BINS]
    return jnp.real(spectrum).astype(jnp.bfloat16), jnp.imag(spectrum).astype(jnp.bfloat16)


def reference(auxiliary, proofs):
    aux_means = jnp.sum(auxiliary, axis=1) / SAMPLES
    wit_means = jnp.sum(proofs, axis=1) / SAMPLES
    wit_real, wit_imag = spectra_of(proofs, wit_means)
    wit_real = wit_real.astype(jnp.float32)
    wit_imag = wit_imag.astype(jnp.float32)
    wit_power = jnp.sum(wit_real * wit_real + wit_imag * wit_imag, axis=1)
    block_size = math.gcd(AUX_CH, 8)
    aux_blocks = auxiliary.reshape(AUX_CH // block_size, block_size, SAMPLES)
    mean_blocks = aux_means.reshape(AUX_CH // block_size, block_size)

    def one_block(block_pair):
        rows_here, block_means = block_pair
        aux_real, aux_imag = spectra_of(rows_here, block_means)
        aux_real = aux_real.astype(jnp.float32)
        aux_imag = aux_imag.astype(jnp.float32)
        cross_real = jnp.einsum("csf,wsf->cwf", aux_real, wit_real) + jnp.einsum("csf,wsf->cwf", aux_imag, wit_imag)
        cross_imag = jnp.einsum("csf,wsf->cwf", aux_imag, wit_real) - jnp.einsum("csf,wsf->cwf", aux_real, wit_imag)
        aux_power = jnp.sum(aux_real * aux_real + aux_imag * aux_imag, axis=1)
        return (cross_real * cross_real + cross_imag * cross_imag) / ((aux_power[:, None, :] + 1e-6) * (wit_power[None, :, :] + 1e-6))

    result = lax.map(one_block, (aux_blocks, mean_blocks))
    return result.reshape(AUX_CH, WIT_CH, BINS)
```

```python
import math, functools
import numpy as np
import jax
import jax.numpy as jnp
from jax import lax
from jax.experimental import pallas as pl
from jax.experimental.pallas import tpu as pltpu
from jax.sharding import PartitionSpec as P

SEG = 8192
STRIDE = 4096
F32 = jnp.float32
BF16 = jnp.bfloat16
ROOT_HALF = math.sqrt(0.5)


def split_table(table):
    high = table.astype(np.float32).astype(BF16)
    low = (table - high.astype(np.float64)).astype(np.float32).astype(BF16)
    return high, low


@functools.cache
def tables():
    q = np.arange(128)
    m = np.arange(64)
    n = np.arange(SEG)
    window = (0.5 - 0.5 * np.cos(2 * np.pi * n / SEG)).reshape(64, 128)
    kp = np.arange(32)
    angle = 2 * np.pi * (kp[:, None] * q[None, :] % SEG) / SEG
    regular = np.zeros((64, 2, 2, 2, 128))
    plus = 2 * np.pi * (m[:, None] * q[None, :] % 128) / 128
    minus = 2 * np.pi * ((127 - m)[:, None] * q[None, :] % 128) / 128
    regular[:, 0, 0, 0] = np.cos(plus)
    regular[:, 0, 0, 1] = np.sin(plus)
    regular[:, 0, 1, 0] = -np.sin(plus)
    regular[:, 0, 1, 1] = np.cos(plus)
    regular[:, 1, 0, 0] = np.cos(minus)
    regular[:, 1, 0, 1] = np.sin(minus)
    regular[:, 1, 1, 0] = np.sin(minus)
    regular[:, 1, 1, 1] = -np.cos(minus)
    packed = np.zeros((64, 2, 2, 2, 128))
    half = 2 * np.pi * ((1 + 2 * m)[:, None] * q[None, :] % 256) / 256
    packed[:, 0, 0, 0] = np.cos(plus)
    packed[:, 0, 1, 0] = -np.sin(plus)
    packed[:, 1, 0, 1] = np.cos(half)
    packed[:, 1, 1, 1] = -np.sin(half)
    weights = []
    for table in (regular, packed):
        high, low = split_table(table.reshape(256, 256))
        weights.append(np.concatenate([high, low], axis=0))
    return (
        window.astype(np.float32),
        np.cos(angle).astype(np.float32),
        np.sin(angle).astype(np.float32),
        np.stack(weights),
    )


def real_dft8(r):
    s0, s1, s2, s3 = (r[i] + r[i + 4] for i in range(4))
    d0, d1, d2, d3 = (r[i] - r[i + 4] for i in range(4))
    e0, e1 = s0 + s2, s1 + s3
    u = ROOT_HALF * (d1 - d3)
    v = ROOT_HALF * (d1 + d3)
    return (
        (e0 + e1, None),
        (d0 + u, -d2 - v),
        (s0 - s2, s3 - s1),
        (d0 - u, d2 - v),
        (e0 - e1, None),
    )


def cadd(a, b):
    return a[0] + b[0], a[1] + b[1]


def csub(a, b):
    return a[0] - b[0], a[1] - b[1]


def mul_minus_i(a):
    return a[1], -a[0]


def complex_dft8(z):
    def dft4(a0, a1, a2, a3):
        s0, d0 = cadd(a0, a2), csub(a0, a2)
        s1, d1 = cadd(a1, a3), csub(a1, a3)
        return (
            cadd(s0, s1),
            (d0[0] + d1[1], d0[1] - d1[0]),
            csub(s0, s1),
            (d0[0] - d1[1], d0[1] + d1[0]),
        )

    even = dft4(z[0], z[2], z[4], z[6])
    odd = dft4(z[1], z[3], z[5], z[7])
    t1 = (ROOT_HALF * (odd[1][0] + odd[1][1]), ROOT_HALF * (odd[1][1] - odd[1][0]))
    t2 = mul_minus_i(odd[2])
    t3 = (ROOT_HALF * (odd[3][1] - odd[3][0]), -ROOT_HALF * (odd[3][0] + odd[3][1]))
    turned = (odd[0], t1, t2, t3)
    return [cadd(even[i], turned[i]) for i in range(4)] + [
        csub(even[i], turned[i]) for i in range(4)
    ]


def spectra_kernel(chans, segs, last_tm, mean_ref, win_ref, cos_ref, sin_ref, w_ref, x_hbm, halo_hbm,
                   out_hbm, xb, yb, ab, s2, ob, in_sem, out_sem):
    s = pl.program_id(0)
    tiles = chans // 8

    def block_copy(block, slot):
        return pltpu.make_async_copy(
            x_hbm.at[:, pl.ds(pl.multiple_of(block * STRIDE, STRIDE), STRIDE)],
            xb.at[slot], in_sem.at[slot])

    def halo_copy(slot):
        return pltpu.make_async_copy(halo_hbm, xb.at[slot], in_sem.at[slot])

    @pl.when(s == 0)
    def _():
        block_copy(0, 0).start()
        block_copy(1, 1).start()
        block_copy(0, 0).wait()

    @pl.when(s + 2 < segs)
    def _():
        block_copy(s + 2, lax.rem(s + 2, 3)).start()

    @pl.when(s + 2 == segs)
    def _():
        halo_copy(lax.rem(s + 2, 3)).start()

    here = lax.rem(s, 3)
    there = lax.rem(s + 1, 3)
    halo_copy(there).wait()

    keep = jnp.where((s == segs - 1) & (lax.axis_index("tm") == last_tm), 0.0, 1.0).astype(F32)

    def octet(o, carry):
        rows = pl.ds(pl.multiple_of(8 * o, 8), 8)
        mean = mean_ref[rows, :]

        def sample(p):
            slot = here if p < 32 else there
            value = xb[slot, rows, 128 * (p % 32): 128 * (p % 32) + 128]
            return value * win_ref[p: p + 1, :]

        for b in range(8):
            y = real_dft8([sample(8 * a + b) for a in range(8)])
            base = 8 * b
            yb[base] = y[0][0]
            for k1 in (1, 2, 3):
                re, im = y[k1]
                if b:
                    c = math.cos(2 * math.pi * b * k1 / 64)
                    d = math.sin(2 * math.pi * b * k1 / 64)
                    re, im = re * c + im * d, im * c - re * d
                yb[base + 2 * k1 - 1] = re
                yb[base + 2 * k1] = im
            yb[base + 7] = y[4][0]

        def put(kp, re, im):
            at = pl.ds(pl.multiple_of(kp * chans + 8 * o, 8), 8)
            ab[at, 0:128] = re
            ab[at, 128:256] = im

        def put_twisted(kp, z, conj):
            c = cos_ref[kp: kp + 1, :]
            d = sin_ref[kp: kp + 1, :]
            if conj:
                put(kp, z[0] * c - z[1] * d, -(z[1] * c + z[0] * d))
            else:
                put(kp, z[0] * c + z[1] * d, z[1] * c - z[0] * d)

        z = real_dft8([yb[8 * b] for b in range(8)])
        put(0, z[0][0] - 32.0 * mean, z[4][0])
        for k2 in (1, 2, 3):
            put_twisted(8 * k2, z[k2], False)
        for k1 in (1, 2, 3):
            z = complex_dft8([(yb[8 * b + 2 * k1 - 1], yb[8 * b + 2 * k1]) for b in range(8)])
            for k2 in range(8):
                k = k1 + 8 * k2
                if k == 1:
                    c = cos_ref[1:2, :]
                    d = sin_ref[1:2, :]
                    put(1, z[0][0] * c + z[0][1] * d + 16.0 * mean, z[0][1] * c - z[0][0] * d)
                elif k < 32:
                    put_twisted(k, z[k2], False)
                else:
                    put_twisted(64 - k, z[k2], True)
        twisted = []
        for b in range(8):
            v = yb[8 * b + 7]
            c = math.cos(2 * math.pi * 4 * b / 64)
            d = math.sin(2 * math.pi * 4 * b / 64)
            twisted.append((v * c, v * -d) if b else (v, jnp.zeros_like(v)))
        z = complex_dft8(twisted)
        for k2 in range(4):
            put_twisted(4 + 8 * k2, z[k2], False)
        return carry

    lax.fori_loop(0, tiles, octet, 0)

    def tile_matmul(v, which):
        a = ab[pl.ds(pl.multiple_of(256 * v, 256), 256), :] * keep
        high = a.astype(BF16)
        low = (a - high.astype(F32)).astype(BF16)
        dims = (((1,), (1,)), ((), ()))
        w_high = w_ref[which, 0:256, :]
        w_low = w_ref[which, 256:512, :]
        left = jnp.concatenate([w_high, w_high, w_low], axis=1)
        right = jnp.concatenate([high, low, high], axis=1)
        return lax.dot_general(left, right, dims, preferred_element_type=F32)

    def store_tile(v, value):
        for half in range(2):
            s2[2 * v + half, pl.ds(s, 256, stride=8), :] = value[:, 128 * half: 128 * half + 128]

    plain = tile_matmul(0, 0)
    packed = tile_matmul(0, 1)
    lane = lax.broadcasted_iota(jnp.int32, (256, 256), 1)
    store_tile(0, jnp.where(lane < chans, packed, plain))
    if tiles > 1:
        def tile(v, carry):
            store_tile(v, tile_matmul(v, 0))
            return carry
        lax.fori_loop(1, tiles, tile, 0)

    @pl.when(s == segs - 1)
    def _():
        def out_copy(u, slot):
            return pltpu.make_async_copy(ob.at[slot], out_hbm.at[:, :, u], out_sem.at[slot])

        for u in range(2 * tiles):
            slot = u % 2
            if u >= 2:
                out_copy(u - 2, slot).wait()
            ob[slot] = s2[u].reshape(16, 8, 16, 128).astype(BF16)
            out_copy(u, slot).start()
        for u in range(max(0, 2 * tiles - 2), 2 * tiles):
            out_copy(u, u % 2).wait()


def local_spectra(x, halo, mean, last_tm):
    chans = x.shape[0]
    segs = x.shape[1] // STRIDE
    window, cos_t, sin_t, weights = tables()
    tiles = chans // 8
    vmem = pl.BlockSpec(memory_space=pltpu.VMEM)
    hbm = pl.BlockSpec(memory_space=pl.ANY)
    return pl.pallas_call(
        functools.partial(spectra_kernel, chans, segs, last_tm),
        grid=(segs,),
        in_specs=[vmem, vmem, vmem, vmem, vmem, hbm, hbm],
        out_specs=hbm,
        out_shape=jax.ShapeDtypeStruct((16, 8, 2 * tiles, 16, 128), BF16),
        scratch_shapes=[
            pltpu.VMEM((3, chans, STRIDE), F32),
            pltpu.VMEM((64, 8, 128), F32),
            pltpu.VMEM((32 * chans, 256), F32),
            pltpu.VMEM((2 * tiles, 2048, 128), F32),
            pltpu.VMEM((2, 16, 8, 16, 128), BF16),
            pltpu.SemaphoreType.DMA((3,)),
            pltpu.SemaphoreType.DMA((2,)),
        ],
        compiler_params=pltpu.CompilerParams(
            dimension_semantics=("arbitrary",), vmem_limit_bytes=56 * 1024 * 1024),
        name="spectra",
    )(mean, jnp.asarray(window), jnp.asarray(cos_t), jnp.asarray(sin_t), jnp.asarray(weights), x, halo)


WIT_STEPS = (0, -2, 2, 4)


def coherence_kernel(aux_ref, *refs):
    wit_refs, (out_ref, wt, zs) = refs[:8], refs[8:]
    mb = pl.program_id(0)
    here = lax.axis_index("chan")
    m = mb // 2
    minus = lax.rem(mb, 2)
    base = here - lax.rem(here, 2)
    side = lax.rem(here, 2)
    for place, wit_ref in enumerate(wit_refs):
        g = lax.rem(base + 8 + WIT_STEPS[place // 2], 8) + (1 - side if place % 2 else side)
        for h in range(2):
            wt[h, g] = wit_ref[:, 0, h].reshape(256, 128).T
    low_lane = lax.broadcasted_iota(jnp.int32, (1, 1, 128), 2) < 64

    def pair(u, carry):
        right = aux_ref[:, 0, u].reshape(256, 128)
        wide = right.astype(F32).reshape(16, 2, 8, 128)
        swapped = jnp.concatenate([wide[:, 1:2], -wide[:, 0:1]], axis=1).reshape(256, 128).astype(BF16)
        aux_power = jnp.sum(jnp.sum(wide * wide, axis=(0, 1)), axis=0, keepdims=True)
        start = pl.multiple_of(16 * lax.rem(u, 8), 16)
        left = wt[u // 8, :, pl.ds(start, 16), :].reshape(128, 256)
        both = jnp.dot(left, jnp.concatenate([right, swapped], axis=1), preferred_element_type=F32)
        left_wide = left.astype(F32)
        wit_power = jnp.sum(left_wide * left_wide, axis=1, keepdims=True).reshape(8, 2, 8, 1)
        cross = (both[:, 0:128] * both[:, 0:128] + both[:, 128:256] * both[:, 128:256]).reshape(8, 2, 8, 128)
        cross = jnp.where(low_lane, cross[:, 0], cross[:, 1])
        wit_power = jnp.where(low_lane, wit_power[:, 0], wit_power[:, 1])
        value = cross / ((aux_power[None] + 1e-6) * (wit_power + 1e-6))
        turned = pltpu.roll(value.reshape(64, 128), 64, 1).reshape(8, 8, 128)
        first = jnp.where(low_lane, value[0:4], turned[4:8]).reshape(32, 128)
        second = jnp.where(low_lane, turned[0:4], value[4:8]).reshape(32, 128)
        kp = 2 * u
        k0 = jnp.where(minus == 1, jnp.where(u == 0, 32, 64 - kp), kp) + 64 * m
        k1 = jnp.where(minus == 1, 63 - kp, kp + 1) + 64 * m
        zs[pl.ds(k0, 32, stride=256), :] = first
        zs[pl.ds(k1, 32, stride=256), :] = second
        return carry

    lax.fori_loop(0, 16, pair, 0)

    @pl.when(mb == 7)
    def _():
        def proof(w, carry):
            for h in range(2):
                start = pl.multiple_of(w * 256 + 128 * h, 128)
                flipped = zs[pl.ds(start, 128), :].T
                out_ref[h, pl.ds(w, 64, stride=64), :] = flipped[0:64]
                out_ref[h, pl.ds(w + 32, 64, stride=64), :] = flipped[64:128]
            return carry
        lax.fori_loop(0, 32, proof, 0)


def local_coherence(aux, wits):
    out = pl.pallas_call(
        coherence_kernel,
        grid=(8,),
        in_specs=[
            pl.BlockSpec((16, 1, 16, 16, 128), lambda i: (0, i, 0, 0, 0)),
        ] + [
            pl.BlockSpec((16, 1, 2, 16, 128), lambda i: (0, i, 0, 0, 0)) for _ in range(8)
        ],
        out_specs=pl.BlockSpec((2, 4096, 128), lambda i: (0, 0, 0)),
        out_shape=jax.ShapeDtypeStruct((2, 4096, 128), F32),
        scratch_shapes=[
            pltpu.VMEM((2, 8, 128, 256), BF16),
            pltpu.VMEM((32 * 256, 128), F32),
        ],
        compiler_params=pltpu.CompilerParams(
            dimension_semantics=("arbitrary",), vmem_limit_bytes=56 * 1024 * 1024),
        name="coherence",
    )(aux, *wits)
    return out.reshape(2, 64, 64, 128).transpose(1, 2, 0, 3).reshape(64, 64, 256)


def swap_pairs(value, flip):
    return lax.ppermute(value, "chan", [(i, i ^ flip) for i in range(8)])


def ring(value, by):
    return lax.ppermute(value, "chan", [(i, (i + by) % 8) for i in range(8)])


def gather_proofs(own):
    other = swap_pairs(own, 1)
    own_left, other_left = ring(own, 2), ring(other, 2)
    own_right, other_right = ring(own, -2), ring(other, -2)
    own_far = ring(own_left, 2)
    other_far = ring(other_right, -2)
    return own, other, own_left, other_left, own_right, other_right, own_far, other_far


def per_device(auxiliary, proofs):
    tm_size = lax.axis_size("tm")
    halo_pairs = [(i, i - 1) for i in range(1, tm_size)]
    wit_halo = lax.ppermute(proofs[:, :STRIDE], "tm", halo_pairs)
    aux_halo = lax.ppermute(auxiliary[:, :STRIDE], "tm", halo_pairs)
    sums = jnp.concatenate([jnp.sum(auxiliary, axis=1), jnp.sum(proofs, axis=1), jnp.zeros((56,), F32)])
    spread = jnp.broadcast_to(sums[None, None, :], (tm_size, 8, 128))
    totals = jnp.sum(lax.all_to_all(spread, "tm", 0, 0, tiled=True)[:, 0], axis=0)
    means = jnp.broadcast_to((totals / (auxiliary.shape[1] * tm_size))[:, None], (128, 128))
    wit_spec = local_spectra(proofs, wit_halo, means[64:72], tm_size - 1)
    wit_moved = lax.all_to_all(wit_spec, "tm", 0, 0, tiled=True)
    wits = gather_proofs(wit_moved)
    aux_spec = local_spectra(auxiliary, aux_halo, means[0:64], tm_size - 1)
    aux_moved = lax.all_to_all(aux_spec, "tm", 0, 0, tiled=True)
    return local_coherence(aux_moved, wits)


def solution(mesh):
    return jax.shard_map(
        per_device,
        mesh=mesh,
        in_specs=(P("chan", "tm"), P("chan", "tm")),
        out_specs=P("chan", None, "tm"),
        check_vma=False,
    )
```
